32 devices in a mesh: groups: 2 (over y), parts: 8 (over z, core), sub: 2 (over x), pair: 1.
Axes of the slice: x: 2, y: 2, z: 4, core: 2. Of those that a mesh axis runs over, the one named last changes fastest.
Arguments:
- spectra: bfloat16 [256, 128, 128], P(('groups', 'parts', 'pair')), parts along dimension 0, may hold values from -6 to 6
- defocus: bfloat16 [256], P(('groups', 'parts', 'pair')), parts along dimension 0, may hold values from 0.5 to 2
- classes: int32 [256, 4], P(('groups', 'parts', 'pair')), parts along dimension 0, may hold values from 0 to 7, all different within a row
- poses: int32 [256, 4], P(('groups', 'parts', 'pair')), parts along dimension 0, may hold values from 0 to 31
- probs: bfloat16 [256, 4], P(('groups', 'parts', 'pair')), parts along dimension 0, may hold values from 0.049804688 to 1
- counts: int32 [16], P(('groups', 'parts', 'pair')), parts along dimension 0, may hold values from 1 to 16, as said below
- offsets: int32 [32], replicated, may hold values from 0 to 64
- row_kernel: bfloat16 [32, 256, 64], P(None, 'sub'), may hold values from -0.015625 to 0.046875
- col_kernel: bfloat16 [32, 128, 64], replicated, may hold values from -0.015625 to 0.046875
Outputs:
- averages: float32 [16, 256, 256], P('groups', ('sub', 'pair')), parts along dimension 0
The draws below stay inside these ranges and needn't reach their ends.
There are 2 independent parts, one for each index of `groups`. The reference program is written for one: setup_inputs(seed, part) draws one part's arguments, and reference() takes and returns one part's arrays. A program takes and returns all parts, laid end to end along the dimension named above; an argument that names none is the same for every part. Nothing has to cross between parts.
Inputs may be any that keep to these rules, and one draw needn't show every extreme that they name: Only the first counts slots of a shard hold used particles; some shard uses all 16 slots. The 4 classes of a particle differ.
All inputs are finite; a program needn't handle non-finite values.
Results may differ from the reference program's by a relative error of at most 0.0038.
Values may be sent and summed in bfloat16 or wider, within the bound.
A program may use at most 64 MiB of HBM per device.

```python
import math
import jax
import jax.numpy as jnp
from jax import lax

GRID = 512
BOX = 256
IROWS = 128
ICOLS = 64
LROWS = 256
LCOLS = 128
BAND = 64
NPOSE = 32
K_TOP = 4
ITERS = 4
P_DEV = 16
SHARDS = 8
PARTICLES = 128
CLASSES = 8
N_PARTS = 8
N_PAIR = 1


def draw_counts(key, part):
    first_key, second_key = jax.random.split(jax.random.fold_in(key, 11))
    drawn = jax.random.randint(first_key, (SHARDS,), 1, P_DEV + 1)
    full_shard = jax.random.randint(second_key, (), 0, SHARDS)
    return jnp.where(jnp.arange(SHARDS) == full_shard, P_DEV, drawn).astype(jnp.int32)


def touch_ends(values, rng, smallest, top_value):
    longest = values.shape.index(max(values.shape))
    spots = []
    for shift in (0, 1):
        where = [jax.random.randint(jax.random.fold_in(rng, axis), (), 0, length) for axis, length in enumerate(values.shape)]
        where[longest] = (where[longest] + shift) % values.shape[longest]
        spots.append(tuple(where))
    return values.at[spots[0]].set(smallest).at[spots[1]].set(top_value)


def shard_levels(stream_key, extent, shards, smallest, high):
    loudness = 1.0
    for dim, parts in shards:
        steps = jax.random.uniform(jax.random.fold_in(jax.random.fold_in(stream_key, 6), dim), (parts,), jnp.float32, smallest / len(shards), high / len(shards))
        loudness = loudness * jnp.repeat(jnp.exp(steps), extent[dim] // parts).reshape((-1,) + (1,) * (len(extent) - 1 - dim))
    return loudness


def picks_of(own_key, rows, count, top, lift):
    sequence = jax.random.permutation(jax.random.fold_in(own_key, 1), count)
    pull = sequence
    for power in range(3):
        pull = pull * pull // count
    pull = pull * lift // count
    lots = jax.random.randint(jax.random.fold_in(own_key, 2), (rows, count), 0, 4096) + pull
    sure = jax.random.permutation(jax.random.fold_in(own_key, 3), rows)[jnp.arange(count) % rows]
    lots = jnp.where(jnp.arange(rows)[:, None] == sure[None, :], 1 << 14, lots)
    merit = lots * count + jnp.arange(count)
    return lax.top_k(merit.astype(jnp.int32), top)[1].astype(jnp.int32)


def scatter_about(key, shape, width, most, cuts=(), held_as=jnp.bfloat16):
    result = jax.random.normal(key, shape, jnp.float32) * width
    if len(cuts) > 0:
        result = shard_levels(key, shape, cuts, -0.22, 0.18) * result
    return jnp.clip(result, min=-most, max=most).astype(held_as)


def setup_inputs(seed: int = 0, part: int = 0) -> dict:
    key_of = jax.random.split(jax.random.key(seed), 10)
    part_keys = jax.random.split(jax.random.fold_in(key_of[9], part), 10)
    spectra = scatter_about(part_keys[0], (PARTICLES, IROWS, 2 * ICOLS), 1.0, 6.0, ((0, 8),))
    defocus = jnp.clip(jnp.exp(math.log(2.0) - 1.3862944 * jax.random.uniform(part_keys[1], (PARTICLES,), jnp.float32) ** shard_levels(part_keys[1], (PARTICLES,), ((0, 8),), -0.2, 0.2)), 0.5, 2.0).astype(jnp.bfloat16)
    classes = picks_of(part_keys[2], PARTICLES, CLASSES, K_TOP, 8192)
    poses = touch_ends(jax.random.randint(part_keys[3], (PARTICLES, K_TOP), 0, NPOSE), jax.random.fold_in(part_keys[3], 1), 0, NPOSE - 1).astype(jnp.int32)
    probs = jnp.clip(jnp.exp(math.log(1.0) - 2.9996462 * jax.random.uniform(part_keys[4], (PARTICLES, K_TOP), jnp.float32) ** shard_levels(part_keys[4], (PARTICLES, K_TOP), ((0, 8),), -0.2, 0.2)), 0.049804688, 1.0).astype(jnp.bfloat16)
    counts = draw_counts(jax.random.fold_in(jax.random.fold_in(key_of[9], part), 71), part)
    offsets = touch_ends(jax.random.randint(key_of[6], (NPOSE,), 0, IROWS - BAND + 1), jax.random.fold_in(key_of[6], 1), 0, IROWS - BAND).astype(jnp.int32)
    row_kernel = jnp.clip(-0.015625 + 0.0625 * jax.random.uniform(key_of[7], (NPOSE, LROWS, BAND), jnp.float32) ** shard_levels(key_of[7], (NPOSE, LROWS, BAND), ((1, 2),), -0.2, 0.2), -0.015625, 0.046875).astype(jnp.bfloat16)
    col_kernel = jnp.clip(jax.random.uniform(key_of[8], (NPOSE, LCOLS, ICOLS), jnp.float32, -0.015625, 0.046875), -0.015625, 0.046875).astype(jnp.bfloat16)
    return dict(spectra=spectra, defocus=defocus, classes=classes, poses=poses, probs=probs, counts=counts, offsets=offsets, row_kernel=row_kernel, col_kernel=col_kernel)


blob_width = 1.5
avg_scale = 8.0
floor_value = 1.0

def ctf_planes(spec_block, defocus_block):
    row_freq = jnp.arange(IROWS, dtype=jnp.float32) - IROWS // 2
    col_freq = jnp.arange(ICOLS, dtype=jnp.float32)
    radius = (row_freq[:, None] ** 2 + col_freq[None, :] ** 2) / (ICOLS * ICOLS)
    phases = 20.0 * math.pi * defocus_block.astype(jnp.float32)[:, None, None] * radius[None] + 0.1
    ctf_value = jnp.sin(phases)
    real_plane = ctf_value * spec_block[:, :, :ICOLS].astype(jnp.float32)
    imag_plane = ctf_value * spec_block[:, :, ICOLS:].astype(jnp.float32)
    return jnp.concatenate([real_plane, imag_plane, ctf_value * ctf_value], axis=2).astype(jnp.bfloat16)

def window_rows(plane_set, start_set):
    return jax.vmap(lambda row_start: lax.dynamic_slice_in_dim(plane_set, row_start, BAND, 0))(start_set)

def block_terms(planes, weights, pose_block, offsets, row_kernel, col_kernel):
    row_starts = offsets[pose_block].astype(jnp.int32)
    windows = jax.vmap(window_rows)(planes, row_starts)
    rows_k = row_kernel[pose_block].astype(jnp.float32)
    cols_k = col_kernel[pose_block].astype(jnp.float32)
    mixed_rows = jnp.einsum('nkrb,nkbj->nkrj', rows_k, windows.astype(jnp.float32), precision=lax.Precision.HIGHEST)
    mixed_rows = (mixed_rows * weights[:, :, None, None]).astype(jnp.bfloat16)
    shape_set = mixed_rows.shape
    mixed_rows = mixed_rows.reshape(shape_set[0], shape_set[1], shape_set[2], 3, ICOLS)
    spread = jnp.einsum('nkrpi,nkci->nkrpc', mixed_rows.astype(jnp.float32), cols_k, precision=lax.Precision.HIGHEST)
    return spread.reshape(shape_set[0] * shape_set[1], shape_set[2], 3 * LCOLS)

def limit_rows():
    return ((jnp.arange(LROWS, dtype=jnp.int32) - LROWS // 2) % GRID).astype(jnp.int32)

def space_from(freq_real, freq_imag):
    row_index = limit_rows()
    col_factor = jnp.where(jnp.arange(LCOLS) == 0, 1.0, 2.0).astype(jnp.float32)
    real_full = jnp.zeros((GRID, GRID), jnp.float32).at[row_index, :LCOLS].set(freq_real * col_factor[None, :])
    imag_full = jnp.zeros((GRID, GRID), jnp.float32).at[row_index, :LCOLS].set(freq_imag * col_factor[None, :])
    return jnp.real(jnp.fft.ifft2(lax.complex(real_full, imag_full))) * GRID

def freq_from(image_field):
    full_freq = jnp.fft.fft2(image_field) / GRID
    picked = full_freq[limit_rows(), :LCOLS]
    return (jnp.real(picked), jnp.imag(picked))

def refine(class_grid):
    grid_index = jnp.arange(GRID, dtype=jnp.int32)
    distance = jnp.minimum(grid_index, GRID - grid_index).astype(jnp.float32)
    blob_axis = jnp.exp(-2.0 * math.pi * math.pi * blob_width * blob_width * distance * distance / (GRID * GRID))
    blob_grid = blob_axis[:, None] * blob_axis[None, :]
    weight_plane = class_grid[:, 2 * LCOLS:]
    rescale = jnp.ones_like(weight_plane)
    for sweep_index in range(ITERS):
        image_field = space_from(weight_plane * rescale, jnp.zeros_like(weight_plane)) * blob_grid
        conv_real, conv_imag = freq_from(image_field)
        rescale = rescale / jnp.maximum(jnp.sqrt(conv_real * conv_real + conv_imag * conv_imag), floor_value)
    image_field = space_from(class_grid[:, :LCOLS] * rescale, class_grid[:, LCOLS:2 * LCOLS] * rescale)
    crop_index = jnp.arange(BOX, dtype=jnp.int32) - BOX // 2
    crop_pos = (crop_index % GRID).astype(jnp.int32)
    correction = jnp.sinc(crop_index.astype(jnp.float32) / GRID) ** 2
    picked = image_field[crop_pos][:, crop_pos]
    return picked.T * avg_scale / (correction[:, None] * correction[None, :])

def reference(spectra, defocus, classes, poses, probs, counts, offsets, row_kernel, col_kernel):
    slot_total = spectra.shape[0]
    per_device = slot_total // (N_PARTS * N_PAIR)
    slot_index = jnp.arange(slot_total, dtype=jnp.int32)
    used_slot = slot_index % per_device < counts[slot_index // per_device]
    weights = probs.astype(jnp.float32) * used_slot.astype(jnp.float32)[:, None]

    def add_block(class_grids, block_index):
        first_slot = (block_index * 8).astype(jnp.int32)
        spec_block = lax.dynamic_slice_in_dim(spectra, first_slot, 8, 0)
        defocus_block = lax.dynamic_slice_in_dim(defocus, first_slot, 8, 0)
        weight_block = lax.dynamic_slice_in_dim(weights, first_slot, 8, 0)
        pose_block = lax.dynamic_slice_in_dim(poses, first_slot, 8, 0)
        class_block = lax.dynamic_slice_in_dim(classes, first_slot, 8, 0)
        planes = ctf_planes(spec_block, defocus_block)
        insert_terms = block_terms(planes, weight_block, pose_block, offsets, row_kernel, col_kernel)
        return (class_grids.at[class_block.reshape(-1)].add(insert_terms), None)
    empty_grid = jnp.zeros((CLASSES, LROWS, 3 * LCOLS), jnp.float32)
    class_grids, unused = lax.scan(add_block, empty_grid, jnp.arange(slot_total // 8, dtype=jnp.int32))
    return lax.map(refine, class_grids)
```

```python
import functools
import math

import jax
import jax.numpy as jnp
import numpy as np
from jax import lax
from jax.experimental import pallas as pl
from jax.experimental.pallas import tpu as pltpu
from jax.sharding import PartitionSpec as P

GRID = 512
BOX = 256
IROWS = 128
ICOLS = 64
LROWS = 256
LCOLS = 128
BAND = 64
ITERS = 4

blob_width = 1.5
avg_scale = 8.0
floor_value = 1.0

f32 = jnp.float32
bf16 = jnp.bfloat16


def split_np(table):
    high = np.asarray(table, np.float32).astype(jnp.bfloat16)
    low = (table - high.astype(np.float64)).astype(np.float32).astype(jnp.bfloat16)
    return np.stack([high, low])


def tables(group_size):
    index = np.arange(GRID)
    distance = np.minimum(index, GRID - index).astype(np.float64)
    blob = np.exp(-2.0 * (math.pi * blob_width * distance / GRID) ** 2)
    beta = (blob[None, :] * np.cos(2 * np.pi * ((index[:, None] * index[None, :]) % GRID) / GRID)).sum(1)
    beta = beta / GRID
    rows = np.arange(LROWS)
    freq = rows - LROWS // 2
    cols = np.arange(LCOLS)
    factor = np.where(cols == 0, 1.0, 2.0)
    row_same = beta[(freq[:, None] - freq[None, :]) % GRID]
    row_flip = beta[(freq[:, None] + freq[None, :]) % GRID]
    row_table = np.concatenate([row_same, row_flip], axis=1)
    col_same = 0.5 * factor[:, None] * beta[(cols[:, None] - cols[None, :]) % GRID]
    col_flip = 0.5 * factor[:, None] * beta[(cols[:, None] + cols[None, :]) % GRID]
    col_table = np.concatenate([col_same, col_flip], axis=1)
    crop = np.arange(BOX) - BOX // 2
    correction = np.sinc(crop / GRID) ** 2
    angles = 2 * np.pi * ((crop[:, None] * cols[None, :]) % GRID) / GRID
    cos_c = factor[None, :] * np.cos(angles) / correction[:, None]
    sin_c = factor[None, :] * np.sin(angles) / correction[:, None]
    first = np.concatenate([cos_c, -sin_c], axis=1).reshape(group_size, -1, 2 * LCOLS)
    second = np.concatenate([sin_c, cos_c], axis=1).reshape(group_size, -1, 2 * LCOLS)
    out_cols = np.concatenate([first, second], axis=1)
    angles = 2 * np.pi * ((freq[:, None] * crop[None, :]) % GRID) / GRID
    scaling = avg_scale / GRID / correction[None, :]
    out_rows = np.concatenate([np.cos(angles) * scaling, -np.sin(angles) * scaling], axis=0)
    out_cols = np.swapaxes(split_np(out_cols), 0, 1)
    return split_np(row_table), split_np(col_table), out_cols, split_np(out_rows)


def sine_turns(turns):
    turns = turns - jnp.round(turns)
    half = jnp.where(turns < 0, -0.5, 0.5)
    turns = jnp.where(jnp.abs(turns) > 0.25, half - turns, turns)
    x = turns * (2.0 * math.pi)
    square = x * x
    value = jnp.full_like(x, -1.0 / math.factorial(11))
    for order in (9, 7, 5, 3, 1):
        sign = 1.0 if order % 4 == 1 else -1.0
        value = value * square + sign / math.factorial(order)
    return value * x


def insert_kernel(
    counts, offsets, classes, poses, spectra, defocus, probs, row_kernel, col_kernel,
    data_out, weight_out, row_pad, col_pad, weights, grids,
):
    slots, top = probs.shape
    pose_count, rows = row_kernel.shape[0], row_kernel.shape[1]
    grids[...] = jnp.zeros_like(grids)
    weights[...] = probs[...].astype(f32)
    band_row = lax.broadcasted_iota(jnp.int32, (BAND, IROWS), 0)
    band_col = lax.broadcasted_iota(jnp.int32, (BAND, IROWS), 1)
    pick_row = lax.broadcasted_iota(jnp.int32, (2 * ICOLS, ICOLS), 0)
    pick_col = lax.broadcasted_iota(jnp.int32, (2 * ICOLS, ICOLS), 1)
    pick_low = (pick_row == pick_col).astype(f32).astype(bf16)
    pick_high = (pick_row == pick_col + ICOLS).astype(f32).astype(bf16)

    def prepare(pose, carry):
        shift = (band_col == band_row + offsets[pose]).astype(f32).astype(bf16)
        placed = jnp.dot(row_kernel[pose], shift, preferred_element_type=f32)
        row_pad[pose] = placed.astype(bf16)
        dims = (((1,), (1,)), ((), ()))
        cols = col_kernel[pose]
        low = lax.dot_general(pick_low, cols, dims, preferred_element_type=f32)
        high = lax.dot_general(pick_high, cols, dims, preferred_element_type=f32)
        col_pad[pose, :, :LCOLS] = low.astype(bf16)
        col_pad[pose, :, LCOLS:] = high.astype(bf16)
        return carry

    lax.fori_loop(0, pose_count, prepare, 0, unroll=4)

    row_freq = lax.broadcasted_iota(jnp.int32, (IROWS, 2 * ICOLS), 0) - IROWS // 2
    col_freq = lax.broadcasted_iota(jnp.int32, (IROWS, 2 * ICOLS), 1) % ICOLS
    radius = (row_freq * row_freq + col_freq * col_freq).astype(f32) * (10.0 / (ICOLS * ICOLS))

    def insert(slot, carry):
        turns = defocus[pl.ds(slot, 1), :] * radius
        turns = turns - jnp.round(turns) + 0.1 / (2.0 * math.pi)
        ctf = sine_turns(turns)
        data = (ctf * spectra[slot].astype(f32)).astype(bf16)
        planes = jnp.concatenate([data, (ctf * ctf).astype(bf16)], axis=1)
        for k in range(top):
            pose = poses[slot, k]
            which = classes[slot, k]
            mixed = jnp.dot(row_pad[pose], planes, preferred_element_type=f32)
            mixed = (mixed * weights[pl.ds(slot, 1), k : k + 1]).astype(bf16)
            stacked = jnp.concatenate([mixed[:, : 2 * ICOLS], mixed[:, 2 * ICOLS :]], axis=0)
            spread = jnp.dot(stacked, col_pad[pose], preferred_element_type=f32)
            grids[which, :, : 2 * LCOLS] += spread[:rows]
            grids[which, :, 2 * LCOLS :] += spread[rows:, :LCOLS]
        return carry

    lax.fori_loop(0, counts[0], insert, 0)
    data_out[...] = grids[:, :, : 2 * LCOLS].astype(bf16)
    weight_out[...] = grids[:, :, 2 * LCOLS :].astype(bf16)


def dot3(a, b, dims=(((1,), (0,)), ((), ()))):
    mul = functools.partial(lax.dot_general, dimension_numbers=dims, preferred_element_type=f32)
    return mul(a[0], b[0]) + (mul(a[0], b[1]) + mul(a[1], b[0]))


def split(value):
    high = value.astype(bf16)
    return high, (value - high.astype(f32)).astype(bf16)


def reduce_kernel(
    sizes, data_part, weight_part, row_hbm, col_hbm, out_cols_hbm, out_rows_hbm, out,
    row_table, col_table, out_cols, out_rows,
    data_mate, data_sum, data_far, data_full, weight_mate, weight_sum, weight_far, weight_full,
    table_sem, mate_send, mate_recv, far_send, far_recv, full_send, full_recv,
    gather_send, gather_recv, pass_send, pass_recv,
):
    parts, sub, pair = sizes
    group = sub * pair
    chips = parts * pair // 2
    part, sub_at, pair_at = (lax.axis_index(axis) for axis in ("parts", "sub", "pair"))
    flat = part * pair + pair_at
    chip = flat // 2
    core = flat % 2
    member = sub_at * pair + pair_at

    def place(index):
        return {"parts": index // pair, "pair": index % pair}

    mate = place(2 * chip + 1 - core)

    def far(step):
        return lax.rem(chip + step, chips)

    def group_place(step):
        index = lax.rem(member + step, group)
        return {"sub": index // pair, "pair": index % pair}

    pieces = ((weight_part, weight_mate, weight_sum, weight_far, weight_full),
              (data_part, data_mate, data_sum, data_far, data_full))

    barrier = pltpu.get_barrier_semaphore()
    peers = [mate] + [place(2 * far(d) + core) for d in range(1, chips)]
    peers += [group_place(e) for e in range(1, group)]
    for peer in peers:
        pl.semaphore_signal(barrier, inc=1, device_id=peer, device_id_type=pl.DeviceIdType.MESH)
    loads = [
        pltpu.make_async_copy(source, target, table_sem.at[i])
        for i, (source, target) in enumerate((
            (row_hbm, row_table), (col_hbm, col_table),
            (out_cols_hbm.at[member], out_cols), (out_rows_hbm, out_rows),
        ))
    ]
    for load in loads:
        load.start()
    pl.semaphore_wait(barrier, len(peers))

    def remote(source, target, send, recv, device):
        return pltpu.make_async_remote_copy(
            src_ref=source, dst_ref=target, send_sem=send, recv_sem=recv,
            device_id=device, device_id_type=pl.DeviceIdType.MESH,
        )

    order = list(range(1, chips)) + [0]
    mate_copies = []
    for t, (local, from_mate, *_) in enumerate(pieces):
        for d in order:
            copy = remote(local.at[2 * far(d) + 1 - core], from_mate.at[d],
                          mate_send.at[t, d], mate_recv.at[t, d], mate)
            copy.start()
            mate_copies.append(copy)
    far_copies = [[], []]
    own = [None, None]
    for t, (local, from_mate, summed, from_far, _) in enumerate(pieces):
        for d in order:
            mate_copies[t * chips + order.index(d)].wait_recv()
            total = local[2 * far(d) + core].astype(f32) + from_mate[d].astype(f32)
            if d == 0:
                own[t] = total
                continue
            summed[d - 1] = total.astype(bf16)
            copy = remote(summed.at[d - 1], from_far.at[d - 1], far_send.at[t, d - 1],
                          far_recv.at[t, d - 1], place(2 * far(d) + core))
            copy.start()
            far_copies[t].append(copy)

    def finish(t):
        _, _, _, from_far, full = pieces[t]
        total = own[t]
        for d in range(1, chips):
            far_copies[t][d - 1].wait_recv()
            total = total + from_far[d - 1].astype(f32)
        full[member] = total.astype(bf16)
        copies = []
        for e in range(1, group):
            copy = remote(full.at[member], full.at[member], full_send.at[t, e - 1],
                          full_recv.at[t, e - 1], group_place(e))
            copy.start()
            copies.append(copy)
        return copies

    def arrive(t):
        full = pieces[t][4]
        for e in range(1, group):
            source = lax.rem(member + group - e, group)
            remote(full.at[source], full.at[source], full_send.at[t, e - 1],
                   full_recv.at[t, e - 1], group_place(e)).wait_recv()
        return full[...].reshape(LROWS, -1).astype(f32)

    group_copies = finish(0)
    loads[0].wait()
    loads[1].wait()
    weight = arrive(0)
    scale = jnp.ones_like(weight)
    rows_split = (row_table[0], row_table[1])
    cols_split = (col_table[0], col_table[1])
    for _ in range(ITERS):
        spread = dot3(split(weight * scale), cols_split)
        spread = jnp.concatenate([spread[:, :LCOLS], spread[:, LCOLS:]], axis=0)
        conv = dot3(rows_split, split(spread))
        scale = scale / jnp.maximum(jnp.abs(conv), floor_value)
    group_copies += finish(1)
    loads[2].wait()
    loads[3].wait()
    data = arrive(1) * jnp.concatenate([scale, scale], axis=1)
    turned = dot3((out_cols[0], out_cols[1]), split(data), (((1,), (1,)), ((), ())))
    block = turned.shape[0] // 2
    turned = jnp.concatenate([turned[:block], turned[block:]], axis=1)
    average = dot3(split(turned), (out_rows[0], out_rows[1]))
    out[part] = average.astype(bf16)

    last = []
    if pair == 1:
        def give(d):
            index = 2 * lax.rem(chip + chips - d, chips) + core
            copy = remote(out.at[index], out.at[index], pass_send.at[d], pass_recv.at[d], mate)
            copy.start()
            last.append(copy)
    for d in range(1, chips):
        copy = remote(out.at[part], out.at[part], gather_send.at[d - 1],
                      gather_recv.at[d - 1], place(2 * far(d) + core))
        copy.start()
        last.append(copy)
    if pair == 1:
        give(0)
    for d in range(1, chips):
        index = (2 * lax.rem(chip + chips - d, chips) + core) // pair
        remote(out.at[index], out.at[index], gather_send.at[d - 1], gather_recv.at[d - 1],
               place(2 * far(d) + core)).wait_recv()
        if pair == 1:
            give(d)
    if pair == 1:
        for d in range(chips):
            index = 2 * lax.rem(chip + chips - d, chips) + 1 - core
            remote(out.at[index], out.at[index], pass_send.at[d], pass_recv.at[d], mate).wait_recv()
    for copy in mate_copies + far_copies[0] + far_copies[1] + group_copies + last:
        copy.wait_send()


def per_device(spectra, defocus, classes, poses, probs, counts, offsets, row_kernel, col_kernel):
    parts, sub, pair = (lax.axis_size(axis) for axis in ("parts", "sub", "pair"))
    group = sub * pair
    count = parts * pair
    chips = count // 2
    rows = row_kernel.shape[1]
    own = rows // pair
    poses_n = row_kernel.shape[0]
    vmem = pl.BlockSpec(memory_space=pltpu.VMEM)
    smem = pl.BlockSpec(memory_space=pltpu.SMEM)
    anywhere = pl.BlockSpec(memory_space=pl.ANY)
    data, weight = pl.pallas_call(
        insert_kernel,
        out_shape=(
            jax.ShapeDtypeStruct((parts, rows, 2 * LCOLS), bf16),
            jax.ShapeDtypeStruct((parts, rows, LCOLS), bf16),
        ),
        in_specs=[smem] * 4 + [vmem] * 5,
        out_specs=(vmem, vmem),
        scratch_shapes=[
            pltpu.VMEM((poses_n, rows, IROWS), bf16),
            pltpu.VMEM((poses_n, 2 * ICOLS, 2 * LCOLS), bf16),
            pltpu.VMEM(probs.shape, f32),
            pltpu.VMEM((parts, rows, 3 * LCOLS), f32),
        ],
        compiler_params=pltpu.CompilerParams(vmem_limit_bytes=40 << 20),
    )(counts, offsets, classes, poses, spectra, defocus.astype(f32).reshape(-1, 1), probs,
      row_kernel, col_kernel)
    data = data.reshape(count, own, 2 * LCOLS)
    weight = weight.reshape(count, own, LCOLS)
    held = tables(group)
    scratch = [pltpu.VMEM(held[i].shape[1:] if i == 2 else held[i].shape, bf16) for i in range(4)]
    for width in (2 * LCOLS, LCOLS):
        scratch += [
            pltpu.VMEM((chips, own, width), bf16),
            pltpu.VMEM((chips - 1, own, width), bf16),
            pltpu.VMEM((chips - 1, own, width), bf16),
            pltpu.VMEM((group, own, width), bf16),
        ]
    scratch.append(pltpu.SemaphoreType.DMA((4,)))
    for shape in ((2, chips), (2, chips - 1), (2, group - 1), (chips - 1,), (chips,)):
        scratch += [pltpu.SemaphoreType.DMA(shape)] * 2
    averages = pl.pallas_call(
        functools.partial(reduce_kernel, (parts, sub, pair)),
        out_shape=jax.ShapeDtypeStruct((parts, BOX // group, BOX), bf16),
        in_specs=[vmem] * 2 + [anywhere] * 4,
        out_specs=vmem,
        scratch_shapes=scratch,
        compiler_params=pltpu.CompilerParams(
            collective_id=0, has_side_effects=True, vmem_limit_bytes=40 << 20
        ),
    )(data, weight, *[jnp.asarray(table) for table in held])
    return averages.astype(f32)


def solution(mesh):
    placed = (
        P(("groups", "parts", "pair"), None, None),
        P(("groups", "parts", "pair")),
        P(("groups", "parts", "pair"), None),
        P(("groups", "parts", "pair"), None),
        P(("groups", "parts", "pair"), None),
        P(("groups", "parts", "pair")),
        P(),
        P(None, "sub", None),
        P(),
    )
    return jax.shard_map(
        per_device,
        mesh=mesh,
        in_specs=placed,
        out_specs=P("groups", ("sub", "pair"), None),
        check_vma=False,
    )
```

```python
import functools
import math

import jax
import jax.numpy as jnp
import numpy as np
from jax import lax
from jax.experimental import pallas as pl
from jax.experimental.pallas import tpu as pltpu
from jax.sharding import PartitionSpec as P

GRID = 512
BOX = 256
IROWS = 128
ICOLS = 64
LROWS = 256
LCOLS = 128
BAND = 64
ITERS = 4

blob_width = 1.5
avg_scale = 8.0
floor_value = 1.0

f32 = jnp.float32
bf16 = jnp.bfloat16


def split_np(table):
    high = np.asarray(table, np.float32).astype(jnp.bfloat16)
    low = (table - high.astype(np.float64)).astype(np.float32).astype(jnp.bfloat16)
    return np.stack([high, low])


def tables(group_size):
    index = np.arange(GRID)
    distance = np.minimum(index, GRID - index).astype(np.float64)
    blob = np.exp(-2.0 * (math.pi * blob_width * distance / GRID) ** 2)
    beta = (blob[None, :] * np.cos(2 * np.pi * ((index[:, None] * index[None, :]) % GRID) / GRID)).sum(1)
    beta = beta / GRID
    rows = np.arange(LROWS)
    freq = rows - LROWS // 2
    cols = np.arange(LCOLS)
    factor = np.where(cols == 0, 1.0, 2.0)
    row_same = beta[(freq[:, None] - freq[None, :]) % GRID]
    row_flip = beta[(freq[:, None] + freq[None, :]) % GRID]
    row_table = np.concatenate([row_same, row_flip], axis=1)
    col_same = 0.5 * factor[:, None] * beta[(cols[:, None] - cols[None, :]) % GRID]
    col_flip = 0.5 * factor[:, None] * beta[(cols[:, None] + cols[None, :]) % GRID]
    col_table = np.concatenate([col_same, col_flip], axis=1)
    crop = np.arange(BOX) - BOX // 2
    correction = np.sinc(crop / GRID) ** 2
    angles = 2 * np.pi * ((crop[:, None] * cols[None, :]) % GRID) / GRID
    cos_c = factor[None, :] * np.cos(angles) / correction[:, None]
    sin_c = factor[None, :] * np.sin(angles) / correction[:, None]
    first = np.concatenate([cos_c, -sin_c], axis=1).reshape(group_size, -1, 2 * LCOLS)
    second = np.concatenate([sin_c, cos_c], axis=1).reshape(group_size, -1, 2 * LCOLS)
    out_cols = np.concatenate([first, second], axis=1)
    angles = 2 * np.pi * ((freq[:, None] * crop[None, :]) % GRID) / GRID
    scaling = avg_scale / GRID / correction[None, :]
    out_rows = np.concatenate([np.cos(angles) * scaling, -np.sin(angles) * scaling], axis=0)
    out_cols = np.swapaxes(split_np(out_cols), 0, 1)
    return split_np(row_table), split_np(col_table), out_cols, split_np(out_rows)


def sine_turns(turns):
    turns = turns - jnp.round(turns)
    half = jnp.where(turns < 0, -0.5, 0.5)
    turns = jnp.where(jnp.abs(turns) > 0.25, half - turns, turns)
    x = turns * (2.0 * math.pi)
    square = x * x
    value = jnp.full_like(x, -1.0 / math.factorial(11))
    for order in (9, 7, 5, 3, 1):
        sign = 1.0 if order % 4 == 1 else -1.0
        value = value * square + sign / math.factorial(order)
    return value * x


def insert_kernel(
    counts, offsets, classes, poses, defocus, probs, spectra, row_kernel, col_kernel,
    data_out, weight_out, row_pad, col_pad, grids,
):
    top, slots = probs.shape
    pose_count, rows = row_kernel.shape[0], row_kernel.shape[2]
    grids[...] = jnp.zeros_like(grids)
    col_pad[...] = jnp.zeros_like(col_pad)
    band_row = lax.broadcasted_iota(jnp.int32, (BAND, IROWS), 0)
    band_col = lax.broadcasted_iota(jnp.int32, (BAND, IROWS), 1)
    band_gap = band_col - band_row

    def prepare(pose, carry):
        shift = (band_gap == offsets[pose]).astype(f32).astype(bf16)
        placed = lax.dot_general(
            row_kernel[pose], shift, (((0,), (0,)), ((), ())), preferred_element_type=f32
        )
        row_pad[pose] = placed.astype(bf16)
        col_pad[pose, :ICOLS, :LCOLS] = col_kernel[pose]
        col_pad[pose, ICOLS:, LCOLS:] = col_kernel[pose]
        return carry

    lax.fori_loop(0, pose_count, prepare, 0, unroll=8)

    row_freq = lax.broadcasted_iota(jnp.int32, (IROWS, 2 * ICOLS), 0) - IROWS // 2
    col_freq = lax.broadcasted_iota(jnp.int32, (IROWS, 2 * ICOLS), 1) % ICOLS
    radius = (row_freq * row_freq + col_freq * col_freq).astype(f32) * (10.0 / (ICOLS * ICOLS))

    def insert(slot, carry):
        used = slot < counts[0]
        turns = defocus[slot] * radius
        turns = turns - jnp.round(turns) + 0.1 / (2.0 * math.pi)
        ctf = sine_turns(turns)
        data = (ctf * spectra[slot].astype(f32)).astype(bf16)
        planes = jnp.concatenate([data, (ctf * ctf).astype(bf16)], axis=1)
        pose_set = [poses[k, slot] for k in range(top)]
        row_set = jnp.concatenate([row_pad[pose] for pose in pose_set], axis=0)
        mixed_set = jnp.dot(row_set, planes, preferred_element_type=f32)
        spread_set = []
        for k, pose in enumerate(pose_set):
            weight = jnp.where(used, probs[k, slot], 0.0)
            mixed = (mixed_set[k * rows : (k + 1) * rows] * weight).astype(bf16)
            stacked = jnp.concatenate([mixed[:, : 2 * ICOLS], mixed[:, 2 * ICOLS :]], axis=0)
            spread_set.append(jnp.dot(stacked, col_pad[pose], preferred_element_type=f32))
        for k, spread in enumerate(spread_set):
            which = classes[k, slot]
            grids[which, :, : 2 * LCOLS] += spread[:rows]
            grids[which, :, 2 * LCOLS :] += spread[rows:, :LCOLS]
        return carry

    lax.fori_loop(0, slots, insert, 0, unroll=2)
    data_out[...] = grids[:, :, : 2 * LCOLS].astype(bf16)
    weight_out[...] = grids[:, :, 2 * LCOLS :].astype(bf16)


def dot3(a, b, dims=(((1,), (0,)), ((), ()))):
    mul = functools.partial(lax.dot_general, dimension_numbers=dims, preferred_element_type=f32)
    return mul(a[0], b[0]) + (mul(a[0], b[1]) + mul(a[1], b[0]))


def split(value):
    high = value.astype(bf16)
    return high, (value - high.astype(f32)).astype(bf16)


def reduce_kernel(
    sizes, data_part, weight_part, row_hbm, col_hbm, out_cols_hbm, out_rows_hbm, out,
    row_table, col_table, out_cols, out_rows,
    data_mate, data_sum, data_far, data_full, weight_mate, weight_sum, weight_far, weight_full,
    table_sem, mate_send, mate_recv, far_send, far_recv, full_send, full_recv,
    gather_send, gather_recv, pass_send, pass_recv,
):
    parts, sub, pair = sizes
    group = sub * pair
    chips = parts * pair // 2
    part, sub_at, pair_at = (lax.axis_index(axis) for axis in ("parts", "sub", "pair"))
    flat = part * pair + pair_at
    chip = flat // 2
    core = flat % 2
    member = sub_at * pair + pair_at

    def place(index):
        return {"parts": index // pair, "pair": index % pair}

    mate = place(2 * chip + 1 - core)

    def far(step):
        return lax.rem(chip + step, chips)

    def group_place(step):
        index = lax.rem(member + step, group)
        return {"sub": index // pair, "pair": index % pair}

    pieces = ((weight_part, weight_mate, weight_sum, weight_far, weight_full),
              (data_part, data_mate, data_sum, data_far, data_full))

    barrier = pltpu.get_barrier_semaphore()
    peers = [mate] + [place(2 * far(d) + core) for d in range(1, chips)]
    peers += [group_place(e) for e in range(1, group)]
    for peer in peers:
        pl.semaphore_signal(barrier, inc=1, device_id=peer, device_id_type=pl.DeviceIdType.MESH)
    loads = [
        pltpu.make_async_copy(source, target, table_sem.at[i])
        for i, (source, target) in enumerate((
            (row_hbm, row_table), (col_hbm, col_table),
            (out_cols_hbm.at[member], out_cols), (out_rows_hbm, out_rows),
        ))
    ]
    for load in loads:
        load.start()
    pl.semaphore_wait(barrier, len(peers))

    def remote(source, target, send, recv, device):
        return pltpu.make_async_remote_copy(
            src_ref=source, dst_ref=target, send_sem=send, recv_sem=recv,
            device_id=device, device_id_type=pl.DeviceIdType.MESH,
        )

    order = list(range(1, chips)) + [0]
    mate_copies = []
    for t, (local, from_mate, *_) in enumerate(pieces):
        for d in order:
            copy = remote(local.at[2 * far(d) + 1 - core], from_mate.at[d],
                          mate_send.at[t, d], mate_recv.at[t, d], mate)
            copy.start()
            mate_copies.append(copy)
    far_copies = [[], []]
    own = [None, None]
    for t, (local, from_mate, summed, from_far, _) in enumerate(pieces):
        for d in order:
            mate_copies[t * chips + order.index(d)].wait_recv()
            total = local[2 * far(d) + core].astype(f32) + from_mate[d].astype(f32)
            if d == 0:
                own[t] = total
                continue
            summed[d - 1] = total.astype(bf16)
            copy = remote(summed.at[d - 1], from_far.at[d - 1], far_send.at[t, d - 1],
                          far_recv.at[t, d - 1], place(2 * far(d) + core))
            copy.start()
            far_copies[t].append(copy)

    def finish(t):
        _, _, _, from_far, full = pieces[t]
        total = own[t]
        for d in range(1, chips):
            far_copies[t][d - 1].wait_recv()
            total = total + from_far[d - 1].astype(f32)
        full[member] = total.astype(bf16)
        copies = []
        for e in range(1, group):
            copy = remote(full.at[member], full.at[member], full_send.at[t, e - 1],
                          full_recv.at[t, e - 1], group_place(e))
            copy.start()
            copies.append(copy)
        return copies

    def arrive(t):
        full = pieces[t][4]
        for e in range(1, group):
            source = lax.rem(member + group - e, group)
            remote(full.at[source], full.at[source], full_send.at[t, e - 1],
                   full_recv.at[t, e - 1], group_place(e)).wait_recv()
        return full[...].reshape(LROWS, -1).astype(f32)

    group_copies = finish(0)
    loads[0].wait()
    loads[1].wait()
    weight = arrive(0)
    scale = jnp.ones_like(weight)
    rows_split = (row_table[0], row_table[1])
    cols_split = (col_table[0], col_table[1])
    for _ in range(ITERS):
        spread = dot3(split(weight * scale), cols_split)
        spread = jnp.concatenate([spread[:, :LCOLS], spread[:, LCOLS:]], axis=0)
        conv = dot3(rows_split, split(spread))
        scale = scale / jnp.maximum(jnp.abs(conv), floor_value)
    group_copies += finish(1)
    loads[2].wait()
    loads[3].wait()
    data = arrive(1) * jnp.concatenate([scale, scale], axis=1)
    turned = dot3((out_cols[0], out_cols[1]), split(data), (((1,), (1,)), ((), ())))
    block = turned.shape[0] // 2
    turned = jnp.concatenate([turned[:block], turned[block:]], axis=1)
    average = dot3(split(turned), (out_rows[0], out_rows[1]))
    out[part] = average.astype(bf16)

    last = []
    if pair == 1:
        def give(d):
            index = 2 * lax.rem(chip + chips - d, chips) + core
            copy = remote(out.at[index], out.at[index], pass_send.at[d], pass_recv.at[d], mate)
            copy.start()
            last.append(copy)
    for d in range(1, chips):
        copy = remote(out.at[part], out.at[part], gather_send.at[d - 1],
                      gather_recv.at[d - 1], place(2 * far(d) + core))
        copy.start()
        last.append(copy)
    if pair == 1:
        give(0)
    for d in range(1, chips):
        index = (2 * lax.rem(chip + chips - d, chips) + core) // pair
        remote(out.at[index], out.at[index], gather_send.at[d - 1], gather_recv.at[d - 1],
               place(2 * far(d) + core)).wait_recv()
        if pair == 1:
            give(d)
    if pair == 1:
        for d in range(chips):
            index = 2 * lax.rem(chip + chips - d, chips) + 1 - core
            remote(out.at[index], out.at[index], pass_send.at[d], pass_recv.at[d], mate).wait_recv()
    for copy in mate_copies + far_copies[0] + far_copies[1] + group_copies + last:
        copy.wait_send()


def per_device(spectra, defocus, classes, poses, probs, counts, offsets, row_kernel, col_kernel):
    parts, sub, pair = (lax.axis_size(axis) for axis in ("parts", "sub", "pair"))
    group = sub * pair
    count = parts * pair
    chips = count // 2
    rows = row_kernel.shape[1]
    own = rows // pair
    poses_n = row_kernel.shape[0]
    vmem = pl.BlockSpec(memory_space=pltpu.VMEM)
    smem = pl.BlockSpec(memory_space=pltpu.SMEM)
    anywhere = pl.BlockSpec(memory_space=pl.ANY)
    data, weight = pl.pallas_call(
        insert_kernel,
        out_shape=(
            jax.ShapeDtypeStruct((parts, rows, 2 * LCOLS), bf16),
            jax.ShapeDtypeStruct((parts, rows, LCOLS), bf16),
        ),
        in_specs=[smem] * 6 + [vmem] * 3,
        out_specs=(vmem, vmem),
        scratch_shapes=[
            pltpu.VMEM((poses_n, rows, IROWS), bf16),
            pltpu.VMEM((poses_n, 2 * ICOLS, 2 * LCOLS), bf16),
            pltpu.VMEM((parts, rows, 3 * LCOLS), f32),
        ],
        compiler_params=pltpu.CompilerParams(vmem_limit_bytes=40 << 20),
    )(counts, offsets, classes.T, poses.T, defocus.astype(f32), probs.T.astype(f32), spectra,
      jnp.swapaxes(row_kernel, 1, 2), jnp.swapaxes(col_kernel, 1, 2))
    data = data.reshape(count, own, 2 * LCOLS)
    weight = weight.reshape(count, own, LCOLS)
    held = tables(group)
    scratch = [pltpu.VMEM(held[i].shape[1:] if i == 2 else held[i].shape, bf16) for i in range(4)]
    for width in (2 * LCOLS, LCOLS):
        scratch += [
            pltpu.VMEM((chips, own, width), bf16),
            pltpu.VMEM((chips - 1, own, width), bf16),
            pltpu.VMEM((chips - 1, own, width), bf16),
            pltpu.VMEM((group, own, width), bf16),
        ]
    scratch.append(pltpu.SemaphoreType.DMA((4,)))
    for shape in ((2, chips), (2, chips - 1), (2, group - 1), (chips - 1,), (chips,)):
        scratch += [pltpu.SemaphoreType.DMA(shape)] * 2
    averages = pl.pallas_call(
        functools.partial(reduce_kernel, (parts, sub, pair)),
        out_shape=jax.ShapeDtypeStruct((parts, BOX // group, BOX), bf16),
        in_specs=[vmem] * 2 + [anywhere] * 4,
        out_specs=vmem,
        scratch_shapes=scratch,
        compiler_params=pltpu.CompilerParams(
            collective_id=0, has_side_effects=True, vmem_limit_bytes=40 << 20
        ),
    )(data, weight, *[jnp.asarray(table) for table in held])
    return averages.astype(f32)


def solution(mesh):
    placed = (
        P(("groups", "parts", "pair"), None, None),
        P(("groups", "parts", "pair")),
        P(("groups", "parts", "pair"), None),
        P(("groups", "parts", "pair"), None),
        P(("groups", "parts", "pair"), None),
        P(("groups", "parts", "pair")),
        P(),
        P(None, "sub", None),
        P(),
    )
    return jax.shard_map(
        per_device,
        mesh=mesh,
        in_specs=placed,
        out_specs=P("groups", ("sub", "pair"), None),
        check_vma=False,
    )
```

```python
import functools
import math

import jax
import jax.numpy as jnp
import numpy as np
from jax import lax
from jax.experimental import pallas as pl
from jax.experimental.pallas import tpu as pltpu
from jax.sharding import PartitionSpec as P

GRID = 512
BOX = 256
IROWS = 128
ICOLS = 64
LROWS = 256
LCOLS = 128
BAND = 64
ITERS = 4

blob_width = 1.5
avg_scale = 8.0
floor_value = 1.0

f32 = jnp.float32
bf16 = jnp.bfloat16

vmem_whole = 67043328
spare = 500 << 10


def split_np(table):
    high = np.asarray(table, np.float32).astype(jnp.bfloat16)
    low = (table - high.astype(np.float64)).astype(np.float32).astype(jnp.bfloat16)
    return np.stack([high, low])


def tables(group_size):
    index = np.arange(GRID)
    distance = np.minimum(index, GRID - index).astype(np.float64)
    blob = np.exp(-2.0 * (math.pi * blob_width * distance / GRID) ** 2)
    beta = (blob[None, :] * np.cos(2 * np.pi * ((index[:, None] * index[None, :]) % GRID) / GRID)).sum(1)
    beta = beta / GRID
    rows = np.arange(LROWS)
    freq = rows - LROWS // 2
    cols = np.arange(LCOLS)
    factor = np.where(cols == 0, 1.0, 2.0)
    row_same = beta[(freq[:, None] - freq[None, :]) % GRID]
    row_flip = beta[(freq[:, None] + freq[None, :]) % GRID]
    row_table = np.concatenate([row_same, row_flip], axis=1)
    col_same = 0.5 * factor[:, None] * beta[(cols[:, None] - cols[None, :]) % GRID]
    col_flip = 0.5 * factor[:, None] * beta[(cols[:, None] + cols[None, :]) % GRID]
    col_table = np.concatenate([col_same, col_flip], axis=1)
    crop = np.arange(BOX) - BOX // 2
    correction = np.sinc(crop / GRID) ** 2
    angles = 2 * np.pi * ((crop[:, None] * cols[None, :]) % GRID) / GRID
    cos_c = factor[None, :] * np.cos(angles) / correction[:, None]
    sin_c = factor[None, :] * np.sin(angles) / correction[:, None]
    first = np.concatenate([cos_c, -sin_c], axis=1).reshape(group_size, -1, 2 * LCOLS)
    second = np.concatenate([sin_c, cos_c], axis=1).reshape(group_size, -1, 2 * LCOLS)
    out_cols = np.concatenate([first, second], axis=1)
    angles = 2 * np.pi * ((freq[:, None] * crop[None, :]) % GRID) / GRID
    scaling = avg_scale / GRID / correction[None, :]
    out_rows = np.concatenate([np.cos(angles) * scaling, -np.sin(angles) * scaling], axis=0)
    out_cols = np.swapaxes(split_np(out_cols), 0, 1)
    return split_np(row_table), split_np(col_table), out_cols, split_np(out_rows)


def sine_turns(turns):
    turns = turns - jnp.round(turns)
    half = jnp.where(turns < 0, -0.5, 0.5)
    turns = jnp.where(jnp.abs(turns) > 0.25, half - turns, turns)
    x = turns * (2.0 * math.pi)
    square = x * x
    value = jnp.full_like(x, -1.0 / math.factorial(11))
    for order in (9, 7, 5, 3, 1):
        sign = 1.0 if order % 4 == 1 else -1.0
        value = value * square + sign / math.factorial(order)
    return value * x


def insert_kernel(
    counts, offsets, classes, poses, defocus, probs, spectra_hbm, row_hbm, col_hbm,
    data_out, weight_out, row_pad, col_pad, grids, spectra, row_kernel, col_kernel, load_sem,
):
    top, slots = probs.shape
    pose_count, rows = row_kernel.shape[0], row_kernel.shape[2]
    loads = [
        pltpu.make_async_copy(source, target, load_sem.at[i])
        for i, (source, target) in enumerate((
            (row_hbm, row_kernel), (col_hbm, col_kernel), (spectra_hbm, spectra),
        ))
    ]
    for load in loads:
        load.start()
    grids[...] = jnp.zeros_like(grids)
    col_pad[...] = jnp.zeros_like(col_pad)
    band_row = lax.broadcasted_iota(jnp.int32, (BAND, IROWS), 0)
    band_col = lax.broadcasted_iota(jnp.int32, (BAND, IROWS), 1)
    band_gap = band_col - band_row

    loads[0].wait()
    loads[1].wait()

    def prepare(pose, carry):
        shift = (band_gap == offsets[pose]).astype(f32).astype(bf16)
        placed = lax.dot_general(
            row_kernel[pose], shift, (((0,), (0,)), ((), ())), preferred_element_type=f32
        )
        row_pad[pose] = placed.astype(bf16)
        col_pad[pose, :ICOLS, :LCOLS] = col_kernel[pose]
        col_pad[pose, ICOLS:, LCOLS:] = col_kernel[pose]
        return carry

    lax.fori_loop(0, pose_count, prepare, 0, unroll=8)

    loads[2].wait()
    row_freq = lax.broadcasted_iota(jnp.int32, (IROWS, 2 * ICOLS), 0) - IROWS // 2
    col_freq = lax.broadcasted_iota(jnp.int32, (IROWS, 2 * ICOLS), 1) % ICOLS
    radius = (row_freq * row_freq + col_freq * col_freq).astype(f32) * (10.0 / (ICOLS * ICOLS))

    def insert(slot, carry):
        used = slot < counts[0]
        turns = defocus[slot] * radius
        turns = turns - jnp.round(turns) + 0.1 / (2.0 * math.pi)
        ctf = sine_turns(turns)
        data = (ctf * spectra[slot].astype(f32)).astype(bf16)
        planes = jnp.concatenate([data, (ctf * ctf).astype(bf16)], axis=1)
        pose_set = [poses[k, slot] for k in range(top)]
        row_set = jnp.concatenate([row_pad[pose] for pose in pose_set], axis=0)
        mixed_set = jnp.dot(row_set, planes, preferred_element_type=f32)
        spread_set = []
        for k, pose in enumerate(pose_set):
            weight = jnp.where(used, probs[k, slot], 0.0)
            mixed = (mixed_set[k * rows : (k + 1) * rows] * weight).astype(bf16)
            stacked = jnp.concatenate([mixed[:, : 2 * ICOLS], mixed[:, 2 * ICOLS :]], axis=0)
            spread_set.append(jnp.dot(stacked, col_pad[pose], preferred_element_type=f32))
        for k, spread in enumerate(spread_set):
            which = classes[k, slot]
            grids[which, :, : 2 * LCOLS] += spread[:rows]
            grids[which, :, 2 * LCOLS :] += spread[rows:, :LCOLS]
        return carry

    lax.fori_loop(0, slots, insert, 0, unroll=2)
    data_out[...] = grids[:, :, : 2 * LCOLS].astype(bf16)
    weight_out[...] = grids[:, :, 2 * LCOLS :].astype(bf16)


def dot3(a, b, dims=(((1,), (0,)), ((), ()))):
    mul = functools.partial(lax.dot_general, dimension_numbers=dims, preferred_element_type=f32)
    return mul(a[0], b[0]) + (mul(a[0], b[1]) + mul(a[1], b[0]))


def split(value):
    high = value.astype(bf16)
    return high, (value - high.astype(f32)).astype(bf16)


def reduce_kernel(
    sizes, data_part, weight_part, row_hbm, col_hbm, out_cols_hbm, out_rows_hbm, out,
    row_table, col_table, out_cols, out_rows,
    data_mate, data_sum, data_far, data_full, weight_mate, weight_sum, weight_far, weight_full,
    table_sem, mate_send, mate_recv, far_send, far_recv, full_send, full_recv,
    gather_send, gather_recv, pass_send, pass_recv,
):
    parts, sub, pair = sizes
    group = sub * pair
    chips = parts * pair // 2
    part, sub_at, pair_at = (lax.axis_index(axis) for axis in ("parts", "sub", "pair"))
    flat = part * pair + pair_at
    chip = flat // 2
    core = flat % 2
    member = sub_at * pair + pair_at

    def place(index):
        return {"parts": index // pair, "pair": index % pair}

    mate = place(2 * chip + 1 - core)

    def far(step):
        return lax.rem(chip + step, chips)

    def group_place(step):
        index = lax.rem(member + step, group)
        return {"sub": index // pair, "pair": index % pair}

    pieces = ((weight_part, weight_mate, weight_sum, weight_far, weight_full),
              (data_part, data_mate, data_sum, data_far, data_full))

    barrier = pltpu.get_barrier_semaphore()
    peers = [mate] + [place(2 * far(d) + core) for d in range(1, chips)]
    peers += [group_place(e) for e in range(1, group)]
    for peer in peers:
        pl.semaphore_signal(barrier, inc=1, device_id=peer, device_id_type=pl.DeviceIdType.MESH)
    loads = [
        pltpu.make_async_copy(source, target, table_sem.at[i])
        for i, (source, target) in enumerate((
            (row_hbm, row_table), (col_hbm, col_table),
            (out_cols_hbm.at[member], out_cols), (out_rows_hbm, out_rows),
        ))
    ]
    for load in loads:
        load.start()
    pl.semaphore_wait(barrier, len(peers))

    def remote(source, target, send, recv, device):
        return pltpu.make_async_remote_copy(
            src_ref=source, dst_ref=target, send_sem=send, recv_sem=recv,
            device_id=device, device_id_type=pl.DeviceIdType.MESH,
        )

    order = list(range(1, chips)) + [0]
    mate_copies = []
    for t, (local, from_mate, *_) in enumerate(pieces):
        for d in order:
            copy = remote(local.at[2 * far(d) + 1 - core], from_mate.at[d],
                          mate_send.at[t, d], mate_recv.at[t, d], mate)
            copy.start()
            mate_copies.append(copy)
    far_copies = [[], []]
    own = [None, None]
    for t, (local, from_mate, summed, from_far, _) in enumerate(pieces):
        for d in order:
            mate_copies[t * chips + order.index(d)].wait_recv()
            total = local[2 * far(d) + core].astype(f32) + from_mate[d].astype(f32)
            if d == 0:
                own[t] = total
                continue
            summed[d - 1] = total.astype(bf16)
            copy = remote(summed.at[d - 1], from_far.at[d - 1], far_send.at[t, d - 1],
                          far_recv.at[t, d - 1], place(2 * far(d) + core))
            copy.start()
            far_copies[t].append(copy)

    def finish(t):
        _, _, _, from_far, full = pieces[t]
        total = own[t]
        for d in range(1, chips):
            far_copies[t][d - 1].wait_recv()
            total = total + from_far[d - 1].astype(f32)
        full[member] = total.astype(bf16)
        copies = []
        for e in range(1, group):
            copy = remote(full.at[member], full.at[member], full_send.at[t, e - 1],
                          full_recv.at[t, e - 1], group_place(e))
            copy.start()
            copies.append(copy)
        return copies

    def arrive(t):
        full = pieces[t][4]
        for e in range(1, group):
            source = lax.rem(member + group - e, group)
            remote(full.at[source], full.at[source], full_send.at[t, e - 1],
                   full_recv.at[t, e - 1], group_place(e)).wait_recv()
        return full[...].reshape(LROWS, -1).astype(f32)

    group_copies = finish(0)
    loads[0].wait()
    loads[1].wait()
    weight = arrive(0)
    scale = jnp.ones_like(weight)
    rows_split = (row_table[0], row_table[1])
    cols_split = (col_table[0], col_table[1])
    for _ in range(ITERS):
        spread = dot3(split(weight * scale), cols_split)
        spread = jnp.concatenate([spread[:, :LCOLS], spread[:, LCOLS:]], axis=0)
        conv = dot3(rows_split, split(spread))
        scale = scale / jnp.maximum(jnp.abs(conv), floor_value)
    group_copies += finish(1)
    loads[2].wait()
    loads[3].wait()
    data = arrive(1) * jnp.concatenate([scale, scale], axis=1)
    turned = dot3((out_cols[0], out_cols[1]), split(data), (((1,), (1,)), ((), ())))
    block = turned.shape[0] // 2
    turned = jnp.concatenate([turned[:block], turned[block:]], axis=1)
    average = dot3(split(turned), (out_rows[0], out_rows[1]))
    out[part] = average.astype(bf16)

    last = []
    if pair == 1:
        def give(d):
            index = 2 * lax.rem(chip + chips - d, chips) + core
            copy = remote(out.at[index], out.at[index], pass_send.at[d], pass_recv.at[d], mate)
            copy.start()
            last.append(copy)
    for d in range(1, chips):
        copy = remote(out.at[part], out.at[part], gather_send.at[d - 1],
                      gather_recv.at[d - 1], place(2 * far(d) + core))
        copy.start()
        last.append(copy)
    if pair == 1:
        give(0)
    for d in range(1, chips):
        index = (2 * lax.rem(chip + chips - d, chips) + core) // pair
        remote(out.at[index], out.at[index], gather_send.at[d - 1], gather_recv.at[d - 1],
               place(2 * far(d) + core)).wait_recv()
        if pair == 1:
            give(d)
    if pair == 1:
        for d in range(chips):
            index = 2 * lax.rem(chip + chips - d, chips) + 1 - core
            remote(out.at[index], out.at[index], pass_send.at[d], pass_recv.at[d], mate).wait_recv()
    for copy in mate_copies + far_copies[0] + far_copies[1] + group_copies + last:
        copy.wait_send()


def per_device(spectra, defocus, classes, poses, probs, counts, offsets, row_kernel, col_kernel):
    parts, sub, pair = (lax.axis_size(axis) for axis in ("parts", "sub", "pair"))
    group = sub * pair
    count = parts * pair
    chips = count // 2
    rows = row_kernel.shape[1]
    own = rows // pair
    poses_n = row_kernel.shape[0]
    partial = 2 * parts * rows * 3 * LCOLS
    result = 2 * parts * (BOX // group) * BOX
    vmem = pl.BlockSpec(memory_space=pltpu.VMEM)
    smem = pl.BlockSpec(memory_space=pltpu.SMEM)
    hbm = pl.BlockSpec(memory_space=pltpu.HBM)
    data, weight = pl.pallas_call(
        insert_kernel,
        out_shape=(
            jax.ShapeDtypeStruct((parts, rows, 2 * LCOLS), bf16),
            jax.ShapeDtypeStruct((parts, rows, LCOLS), bf16),
        ),
        in_specs=[smem] * 6 + [hbm] * 3,
        out_specs=(vmem, vmem),
        scratch_shapes=[
            pltpu.VMEM((poses_n, rows, IROWS), bf16),
            pltpu.VMEM((poses_n, 2 * ICOLS, 2 * LCOLS), bf16),
            pltpu.VMEM((parts, rows, 3 * LCOLS), f32),
            pltpu.VMEM(spectra.shape, bf16),
            pltpu.VMEM((poses_n, BAND, rows), bf16),
            pltpu.VMEM((poses_n, ICOLS, LCOLS), bf16),
            pltpu.SemaphoreType.DMA((3,)),
        ],
        compiler_params=pltpu.CompilerParams(vmem_limit_bytes=vmem_whole - partial - spare),
    )(counts, offsets, classes.T, poses.T, defocus.astype(f32), probs.T.astype(f32), spectra,
      jnp.swapaxes(row_kernel, 1, 2), jnp.swapaxes(col_kernel, 1, 2))
    data = data.reshape(count, own, 2 * LCOLS)
    weight = weight.reshape(count, own, LCOLS)
    held = tables(group)
    scratch = [pltpu.VMEM(held[i].shape[1:] if i == 2 else held[i].shape, bf16) for i in range(4)]
    for width in (2 * LCOLS, LCOLS):
        scratch += [
            pltpu.VMEM((chips, own, width), bf16),
            pltpu.VMEM((chips - 1, own, width), bf16),
            pltpu.VMEM((chips - 1, own, width), bf16),
            pltpu.VMEM((group, own, width), bf16),
        ]
    scratch.append(pltpu.SemaphoreType.DMA((4,)))
    for shape in ((2, chips), (2, chips - 1), (2, group - 1), (chips - 1,), (chips,)):
        scratch += [pltpu.SemaphoreType.DMA(shape)] * 2
    averages = pl.pallas_call(
        functools.partial(reduce_kernel, (parts, sub, pair)),
        out_shape=jax.ShapeDtypeStruct((parts, BOX // group, BOX), bf16),
        in_specs=[vmem] * 2 + [hbm] * 4,
        out_specs=vmem,
        scratch_shapes=scratch,
        compiler_params=pltpu.CompilerParams(
            collective_id=0, has_side_effects=True, vmem_limit_bytes=vmem_whole - partial - result - spare
        ),
    )(data, weight, *[jnp.asarray(table) for table in held])
    return averages.astype(f32)


def solution(mesh):
    placed = (
        P(("groups", "parts", "pair"), None, None),
        P(("groups", "parts", "pair")),
        P(("groups", "parts", "pair"), None),
        P(("groups", "parts", "pair"), None),
        P(("groups", "parts", "pair"), None),
        P(("groups", "parts", "pair")),
        P(),
        P(None, "sub", None),
        P(),
    )
    return jax.shard_map(
        per_device,
        mesh=mesh,
        in_specs=placed,
        out_specs=P("groups", ("sub", "pair"), None),
        check_vma=False,
    )
```
